32 devices in a mesh: band: 4 (over z), ga: 8 (over y, x, core).
Axes of the slice: x: 2, y: 2, z: 4, core: 2. Of those that a mesh axis runs over, the one named last changes fastest.
Arguments:
- waves: bfloat16 [2, 128, 8192], P(None, 'band', 'ga'), may hold values from -6 to 6
- occupations: float32 [128], P('band'), may hold values from 0.0015625 to 0.03125
- beta_table: float32 [72, 8192], P(None, 'ga'), may hold values from -0.046875 to 0.046875
- wave_miller: int32 [3, 8192], P(None, 'ga'), may hold values from 0 to 223
- atom_kinds: int32 [256], replicated, may hold values from 0 to 3
- atom_sites: int32 [3, 256], replicated, may hold values from 0 to 223
- aug_table: bfloat16 [684, 57344], P(None, ('band', 'ga')), may hold values from -0.00061035156 to 0.00061035156
- stick_columns: int32 [256], P(('band', 'ga')), may hold values from -1 to 14399, as said below
Outputs:
- density: float32 [2, 224, 240, 240], P(None, 'ga', 'band')
The draws below stay inside these ranges and needn't reach their ends.
Inputs may be any that keep to these rules, and one draw needn't show every extreme that they name: `stick_columns`: entry t is a slot of the device at place t // 8 in band-major order, of band index t // 64. -1 marks an empty slot; otherwise the entry c names the column x = (t // 64) * 60 + c // 240, y = c mod 240. Live columns of one band index are distinct. On each device the live slots come first and at least one is live; in each band index some device has all 8 slots live.
All inputs are finite; a program needn't handle non-finite values.
Results may differ from the reference program's by a relative error of at most 0.0035.
Values sent between devices are 32-bit elements; how exact they have to be, the bound alone decides.
A program may use at most 64 MiB of HBM per device.

```python
import math
import jax
import jax.numpy as jnp
import numpy as np
from jax import lax

NX = 240
NY = 240
NZ = 224
NH = 18
PAIRS = 171
SPECIES = 4
ATOMS = 256
BANDS = 128
GW = 8192
STK = 8
STICKS = 256
BLOCK_STICKS = 64
NXB = 60


def draw_stick_columns(key, part):
    groups = STICKS // BLOCK_STICKS
    devices = BLOCK_STICKS // STK
    group_keys = jax.random.split(jax.random.fold_in(key, 11), groups)

    def one_group(group_key):
        perm_key, count_key, full_key = jax.random.split(group_key, 3)
        chosen = jax.random.permutation(perm_key, NXB * NY)[:BLOCK_STICKS].astype(jnp.int32).reshape(devices, STK)
        live_count = jax.random.randint(count_key, (devices,), 1, STK // 2 + 1)
        fullest = jax.random.randint(full_key, (), 0, devices)
        live_count = jnp.where(jnp.arange(devices) == fullest, STK, live_count)
        slot_index = jnp.arange(STK)[None, :]
        return jnp.where(slot_index < live_count[:, None], chosen, -1).reshape(-1)
    return jax.vmap(one_group)(group_keys).reshape(-1).astype(jnp.int32)


def place_ends(values, own_key, least, high):
    longest = values.shape.index(max(values.shape))
    spots = []
    for shift in (0, 1):
        where = [jax.random.randint(jax.random.fold_in(own_key, axis), (), 0, length) for axis, length in enumerate(values.shape)]
        where[longest] = (where[longest] + shift) % values.shape[longest]
        spots.append(tuple(where))
    return values.at[spots[0]].set(least).at[spots[1]].set(high)


def levels(stream_key, extent, shards, low, top_value):
    level = 1.0
    for position, parts in shards:
        heights = jax.random.uniform(jax.random.fold_in(jax.random.fold_in(stream_key, 6), position), (parts,), jnp.float32, low / len(shards), top_value / len(shards))
        level = level * jnp.repeat(jnp.exp(heights), extent[position] // parts).reshape((-1,) + (1,) * (len(extent) - 1 - position))
    return level


def centred(key, extent, spread, limit, cuts=(), held_as=jnp.bfloat16):
    values = jax.random.normal(key, extent, jnp.float32) * spread
    if len(cuts) > 0:
        values = levels(key, extent, cuts, -0.22, 0.18) * values
    return jnp.clip(values, min=-limit, max=limit).astype(held_as)


def setup_inputs(seed: int = 0) -> dict:
    key_of = jax.random.split(jax.random.key(seed), 9)
    return {
        "waves": centred(key_of[0], (2, BANDS, GW), 1.0, 6.0, ((1, 4), (2, 8))),
        "occupations": jnp.clip(jnp.exp(math.log(0.03125) - 2.9957323 * jax.random.uniform(key_of[1], (BANDS,), jnp.float32) ** levels(key_of[1], (BANDS,), ((0, 4),), -0.2, 0.2)), 0.0015625, 0.03125),
        "beta_table": centred(key_of[2], (SPECIES * NH, GW), (2 * GW) ** -0.5, 0.046875, ((1, 8),), jnp.float32),
        "wave_miller": place_ends(jax.random.randint(key_of[3], (3, GW), 0, min(NX, min(NY, NZ))), jax.random.fold_in(key_of[3], 1), 0, (min(NX, min(NY, NZ))) - 1).astype(jnp.int32),
        "atom_kinds": place_ends(jax.random.randint(key_of[4], (ATOMS,), 0, SPECIES), jax.random.fold_in(key_of[4], 1), 0, SPECIES - 1).astype(jnp.int32),
        "atom_sites": place_ends(jax.random.randint(key_of[5], (3, ATOMS), 0, min(NX, min(NY, NZ))), jax.random.fold_in(key_of[5], 1), 0, (min(NX, min(NY, NZ))) - 1).astype(jnp.int32),
        "aug_table": centred(key_of[6], (SPECIES * PAIRS, STICKS * NZ), ((40.0 * ATOMS * STICKS * NZ) ** -0.5), 0.00061035156, ((1, 32),)),
        "stick_columns": draw_stick_columns(jax.random.fold_in(key_of[8], 71), 0),
    }


highest = lax.Precision.HIGHEST


def pair_tables(proj_count):
    ell_values = np.array([0, 0] + [1] * 6 + [2] * 10)
    pair_first, pair_second = np.triu_indices(proj_count)
    factors = np.where(pair_first == pair_second, 1.0, 2.0).astype(np.float32)
    parity = ((ell_values[pair_first] + ell_values[pair_second]) % 2).astype(np.float32)
    return pair_first * proj_count + pair_second, factors, parity


def phase_coefficients():
    ell_values = np.array([0, 0] + [1] * 6 + [2] * 10)
    coef_real = np.array([1.0, 0.0, -1.0])[ell_values]
    coef_imag = np.array([0.0, -1.0, 0.0])[ell_values]
    return jnp.asarray(coef_real, jnp.float32), jnp.asarray(coef_imag, jnp.float32)


def phase_angle(site_block, first, second, third):
    turn_count = ((site_block[0][:, None] * first[None, :]) % NX) * (NY * NZ)
    turn_count = turn_count + ((site_block[1][:, None] * second[None, :]) % NY) * (NX * NZ)
    turn_count = turn_count + ((site_block[2][:, None] * third[None, :]) % NZ) * (NX * NY)
    turn_count = (turn_count % (NX * NY * NZ)).astype(jnp.int32)
    angle_value = turn_count.astype(jnp.float32) * (2.0 * np.pi / (NX * NY * NZ))
    return jnp.cos(angle_value), -jnp.sin(angle_value)


def structure_factor(site_block, miller):
    return phase_angle(site_block, miller[0], miller[1], miller[2])


def projector_rows(site_block, kinds_block, beta_table, wave_miller):
    struct_re, struct_im = structure_factor(site_block, wave_miller)
    kind_onehot = (kinds_block[:, None] == jnp.arange(SPECIES, dtype=jnp.int32)[None, :]).astype(jnp.float32)
    table_three = beta_table.reshape(SPECIES, NH, -1)
    radial = jnp.einsum("as,sig->aig", kind_onehot, table_three, precision=highest)
    coef_real, coef_imag = phase_coefficients()
    part_re = radial * struct_re[:, None, :]
    part_im = radial * struct_im[:, None, :]
    vkb_re = coef_real[None, :, None] * part_re - coef_imag[None, :, None] * part_im
    vkb_im = coef_real[None, :, None] * part_im + coef_imag[None, :, None] * part_re
    return vkb_re.astype(jnp.bfloat16), vkb_im.astype(jnp.bfloat16)


def augment_weights(becsum, atom_kinds):
    pair_index, factors, parity = pair_tables(NH)
    kind_onehot = (atom_kinds[None, :] == jnp.arange(SPECIES, dtype=jnp.int32)[:, None]).astype(jnp.float32)
    parity_col = jnp.asarray(parity, jnp.float32)[:, None]
    even_rows = becsum.T * (1.0 - parity_col)
    odd_rows = -(becsum.T * parity_col)
    real_part = kind_onehot[:, None, :] * even_rows[None, :, :]
    imag_part = kind_onehot[:, None, :] * odd_rows[None, :, :]
    stacked = jnp.concatenate([real_part, imag_part], axis=2)
    return stacked.reshape(-1, stacked.shape[2]).astype(jnp.bfloat16)


def dense_augmentation(coefficients, atom_sites, column_x, column_y):
    slot_total = column_x.shape[0]
    zeros_z = jnp.zeros((1, NZ), jnp.int32)
    flat_x = (column_x[:, None] + zeros_z).reshape(-1).astype(jnp.int32)
    flat_y = (column_y[:, None] + zeros_z).reshape(-1).astype(jnp.int32)
    flat_z = (jnp.zeros((slot_total, 1), jnp.int32) + jnp.arange(NZ, dtype=jnp.int32)[None, :]).reshape(-1)
    struct_re, struct_im = phase_angle(atom_sites, flat_x, flat_y, flat_z)
    atom_total = coefficients.shape[0] // 2
    amp_re = coefficients[:atom_total]
    amp_im = coefficients[atom_total:]
    aug_re = jnp.sum(amp_re * struct_re - amp_im * struct_im, axis=0)
    aug_im = jnp.sum(amp_re * struct_im + amp_im * struct_re, axis=0)
    return aug_re.reshape(slot_total, NZ), aug_im.reshape(slot_total, NZ)


def reference(waves, occupations, beta_table, wave_miller, atom_kinds, atom_sites, aug_table, stick_columns):
    block_atoms = math.gcd(ATOMS, 8)
    wave_re = waves[0].astype(jnp.float32).T
    wave_im = waves[1].astype(jnp.float32).T

    def project_block(block_index):
        first_atom = block_index * block_atoms
        site_block = lax.dynamic_slice_in_dim(atom_sites, first_atom, block_atoms, 1)
        kinds_block = lax.dynamic_slice_in_dim(atom_kinds, first_atom, block_atoms, 0)
        vkb_re, vkb_im = projector_rows(site_block, kinds_block, beta_table, wave_miller)
        vkb_re = vkb_re.reshape(block_atoms * NH, -1).astype(jnp.float32)
        vkb_im = vkb_im.reshape(block_atoms * NH, -1).astype(jnp.float32)
        proj_re = jnp.dot(vkb_re, wave_re, precision=highest, preferred_element_type=jnp.float32) + jnp.dot(vkb_im, wave_im, precision=highest, preferred_element_type=jnp.float32)
        proj_im = jnp.dot(vkb_re, wave_im, precision=highest, preferred_element_type=jnp.float32) - jnp.dot(vkb_im, wave_re, precision=highest, preferred_element_type=jnp.float32)
        return proj_re.reshape(block_atoms, NH, -1), proj_im.reshape(block_atoms, NH, -1)

    becp_re, becp_im = lax.map(project_block, jnp.arange(ATOMS // block_atoms, dtype=jnp.int32))
    becp_re = becp_re.reshape(ATOMS, NH, -1)
    becp_im = becp_im.reshape(ATOMS, NH, -1)
    full_square = jnp.einsum("aic,ajc->aij", becp_re * occupations[None, None, :], becp_re, precision=highest)
    full_square = full_square + jnp.einsum("aic,ajc->aij", becp_im * occupations[None, None, :], becp_im, precision=highest)
    pair_index, factors, parity = pair_tables(NH)
    becsum = full_square.reshape(ATOMS, NH * NH)[:, pair_index] * factors[None, :]

    aug_weights = augment_weights(becsum, atom_kinds).astype(jnp.float32)
    stick_block = math.gcd(STICKS, 16)

    def dense_block(block_index):
        first_stick = block_index * stick_block
        columns = lax.dynamic_slice_in_dim(stick_columns, first_stick, stick_block, 0)
        table_block = lax.dynamic_slice_in_dim(aug_table, first_stick * NZ, stick_block * NZ, 1).astype(jnp.float32)
        stick_ids = first_stick + jnp.arange(stick_block, dtype=jnp.int32)
        column_x = (stick_ids // BLOCK_STICKS) * NXB + columns // NY
        column_y = columns % NY
        coefficients = jnp.dot(aug_weights.T, table_block, precision=highest, preferred_element_type=jnp.float32)
        aug_re, aug_im = dense_augmentation(coefficients, atom_sites, column_x, column_y)
        flat_rows = jnp.where(columns < 0, NX * NY, column_x * NY + column_y).astype(jnp.int32)
        return aug_re, aug_im, flat_rows

    aug_re, aug_im, flat_rows = lax.map(dense_block, jnp.arange(STICKS // stick_block, dtype=jnp.int32))
    flat_rows = flat_rows.reshape(-1)
    grid_re = jnp.zeros((NX * NY, NZ), jnp.float32).at[flat_rows].add(aug_re.reshape(-1, NZ), mode="drop")
    grid_im = jnp.zeros((NX * NY, NZ), jnp.float32).at[flat_rows].add(aug_im.reshape(-1, NZ), mode="drop")
    grid_values = lax.complex(grid_re, grid_im).reshape(NX, NY, NZ)
    density_field = jnp.fft.ifftn(grid_values) * (NX * NY * NZ)
    density_field = jnp.transpose(density_field, (2, 1, 0))
    return jnp.stack([jnp.real(density_field), jnp.imag(density_field)]).astype(jnp.float32)
```

```python
import functools
import math

import jax
import jax.numpy as jnp
import numpy as np
from jax import lax
from jax.experimental import pallas as pl
from jax.experimental.pallas import tpu as pltpu
from jax.sharding import PartitionSpec as P

NX = 240
NY = 240
NZ = 224
NH = 18
HALF = NH // 2
SPECIES = 4

PERIOD = math.lcm(NX, NY, NZ)
STEP_X = PERIOD // NX
STEP_Y = PERIOD // NY
STEP_Z = PERIOD // NZ
ELL = np.array([0, 0] + [1] * 6 + [2] * 10)
PAIR_FIRST, PAIR_SECOND = np.triu_indices(NH)

highest = lax.Precision.HIGHEST
F32 = jnp.float32
BF16 = jnp.bfloat16


def fit_even(func, terms):
    nodes = 0.125 * (1.0 + np.cos(np.pi * (np.arange(64) + 0.5) / 64))
    scaled = np.polynomial.chebyshev.Chebyshev.fit(nodes, func(np.sqrt(nodes)), terms - 1, domain=[0, 0.25])
    return [float(c) for c in scaled.convert(kind=np.polynomial.Polynomial).coef]


COS_FIT = fit_even(lambda u: np.cos(2 * np.pi * u), 7)
SIN_FIT = fit_even(lambda u: np.sin(2 * np.pi * u) / u, 6)


def horner(coefs, w):
    total = jnp.full_like(w, coefs[-1])
    for c in coefs[-2::-1]:
        total = total * w + c
    return total


def turn_cos_sin(count, period):
    rest = count - jnp.round(count * (1.0 / period)) * period
    u = rest * (1.0 / period)
    w = u * u
    return horner(COS_FIT, w), u * horner(SIN_FIT, w)


MESH = pl.DeviceIdType.MESH


def greet(peers, axis_sets):
    barrier = pltpu.get_barrier_semaphore()
    for count, device_of in axis_sets:

        @pl.loop(1, count)
        def _(step):
            pl.semaphore_signal(barrier, inc=1, device_id=device_of(step), device_id_type=MESH)

    return lambda: pl.semaphore_wait(barrier, peers)


def up(value, unit):
    return -(-value // unit) * unit


def split(value):
    high = value.astype(BF16)
    return high, (value - high.astype(F32)).astype(BF16)


def mixed(value, other, count):
    if count & (count - 1):
        return lax.rem(value + other, count)
    total, bit = 0, 1
    while bit < count:
        total = total + lax.rem(value // bit + other // bit, 2) * bit
        bit *= 2
    return total


def mega_kernel(
    bands,
    groups,
    waves_hbm,
    occ_hbm,
    beta_hbm,
    miller_hbm,
    kinds_hbm,
    site_hbm,
    columns_hbm,
    signs_hbm,
    table_hbm,
    spread_hbm,
    out_ref,
    waves_ref,
    occ_ref,
    beta_ref,
    miller_ref,
    kinds_ref,
    site_ref,
    columns_ref,
    signs_ref,
    small_ref,
    site_t_ref,
    radial_ref,
    wave_ref,
    rows_ref,
    send_ref,
    mate_ref,
    recv_ref,
    phase_ref,
    total_ref,
    part_ref,
    band_ref,
    pair_ref,
    pack_ref,
    sum_ref,
    all_ref,
    weights_ref,
    table_ref,
    spread_ref,
    aug_ref,
    lines_ref,
    stick_ref,
    mate_send,
    mate_recv,
    rs_send,
    rs_recv,
    band_send,
    band_recv,
    ga_send,
    ga_recv,
    dev_send,
    dev_recv,
    local_sem,
):
    band, me = lax.axis_index("band"), lax.axis_index("ga")
    devices = bands * groups
    place = band * groups + me
    chips = groups // 2
    chip, core = me // 2, lax.rem(me, 2)
    atoms = site_ref.shape[1]
    own = atoms // groups
    width = miller_ref.shape[1]
    nb = waves_ref.shape[1]
    slots = columns_ref.shape[0]
    steps, _, block, cols = send_ref.shape
    ratio = block // own
    paired = ratio == 1
    rounds = steps // 2 if paired else steps
    units = max(1, ratio // 2)
    points = slots * NZ
    tile = phase_ref.shape[-1]
    planes = NZ // groups
    rows, lanes = stick_ref.shape[1:]
    span = lanes * rows // slots
    pairs = len(PAIR_FIRST)

    sources = (site_hbm, kinds_hbm, occ_hbm, waves_hbm, miller_hbm, beta_hbm, columns_hbm, signs_hbm, table_hbm, spread_hbm)
    targets = (site_ref, kinds_ref, occ_ref, waves_ref, miller_ref, beta_ref, columns_ref, signs_ref, table_ref, spread_ref)
    loads = [pltpu.make_async_copy(a, b, local_sem.at[n]) for n, (a, b) in enumerate(zip(sources, targets))]
    for load in loads:
        load.start()

    all_here = greet(
        groups - 1 + bands - 1,
        [
            (groups, lambda step: (band, lax.rem(me + step, groups))),
            (bands, lambda step: (lax.rem(band + step, bands), me)),
        ],
    )

    wave_ref[...] = jnp.zeros_like(wave_ref)
    small_ref[...] = jnp.zeros_like(small_ref)
    for load in loads[:3]:
        load.wait()
    small_ref[0:1, :] = site_ref[0:1, :].astype(F32) * STEP_X
    small_ref[1:2, :] = site_ref[1:2, :].astype(F32) * STEP_Y
    small_ref[2:3, :] = site_ref[2:3, :].astype(F32) * STEP_Z
    small_ref[3:4, :] = kinds_ref[...].astype(F32)
    small_ref[4:5, 0:nb] = occ_ref[...]
    small_ref[4:5, nb : 2 * nb] = occ_ref[...]
    site_t_ref[...] = jnp.swapaxes(small_ref[...], 0, 1)

    loads[3].wait()
    re, im = waves_ref[0], waves_ref[1]
    for h in range(2):
        r, c = 2 * nb * h, 2 * width * h
        wave_ref[r : r + nb, c : c + width] = re
        wave_ref[r : r + nb, c + width : c + 2 * width] = im
        wave_ref[r + nb : r + 2 * nb, c : c + width] = im
        wave_ref[r + nb : r + 2 * nb, c + width : c + 2 * width] = -re
    loads[4].wait()
    loads[5].wait()
    for i in range(NH):
        for s in range(SPECIES):
            row = (i // HALF) * SPECIES + s
            radial_ref[i % HALF, row : row + 1, :] = beta_ref[s * NH + i : s * NH + i + 1, :]

    def located(turn, unit, own_core):
        kind = core if own_core else 1 - core
        if paired:
            target = mixed(chip, rounds - 1 - turn, rounds) * 2 + kind
            return target, 0, target
        index = mixed(me // ratio, rounds - 1 - turn, rounds)
        part = 2 * unit + kind
        return index, pl.multiple_of(part * own, own), index * ratio + part

    def mate_copy(index, offset, slot):
        return pltpu.make_async_remote_copy(
            src_ref=send_ref.at[index, :, pl.ds(offset, own), :],
            dst_ref=mate_ref.at[slot],
            send_sem=mate_send.at[slot],
            recv_sem=mate_recv.at[slot],
            device_id=(band, chip * 2 + 1 - core),
            device_id_type=MESH,
        )

    def rs_copy(index, offset, target, slot):
        return pltpu.make_async_remote_copy(
            src_ref=send_ref.at[index, :, pl.ds(offset, own), :],
            dst_ref=recv_ref.at[slot],
            send_sem=rs_send.at[target],
            recv_sem=rs_recv.at[slot],
            device_id=(band, target * 2 + core),
            device_id_type=MESH,
        )

    def project(index):
        start = pl.multiple_of(index * block, block)
        site = site_t_ref[pl.ds(start, block), :]
        kinds = site[:, 3:4]
        miller = miller_ref[...].astype(F32)
        count = site[:, 0:1] * miller[0:1, :] + site[:, 1:2] * miller[1:2, :] + site[:, 2:3] * miller[2:3, :]
        cosine, sine = turn_cos_sin(count, PERIOD)
        minus = -sine
        kinds8 = [
            [jnp.broadcast_to(kinds[q : q + 8] + float(SPECIES * h), (8, width)).astype(jnp.int32) for q in range(0, block, 8)]
            for h in range(2)
        ]
        for i in range(NH):
            radial = jnp.concatenate(
                [
                    jnp.take_along_axis(
                        radial_ref[i % HALF],
                        kinds8[i // HALF][q],
                        axis=0,
                        mode="promise_in_bounds",
                    )
                    for q in range(block // 8)
                ],
                axis=0,
            )
            first, second = (sine, cosine) if ELL[i] == 1 else (cosine, minus)
            row = (i % HALF) * block
            col = (i // HALF) * 2 * width
            rows_ref[row : row + block, col : col + width] = (radial * first).astype(BF16)
            rows_ref[row : row + block, col + width : col + 2 * width] = (radial * second).astype(BF16)
        result = lax.dot_general(
            rows_ref[...], wave_ref[...], (((1,), (1,)), ((), ())), preferred_element_type=F32
        )
        send_ref[index] = result.reshape(HALF, block, cols)

    def forward(turn):
        for unit in range(units):
            index, offset, target = located(turn, unit, False)
            mate_copy(index, offset, target // 2).start()

    def settle(turn):
        for unit in range(units):
            index, offset, target = located(turn, unit, True)
            mate_copy(index, offset, target // 2).wait_recv()
            here = (index, slice(None), pl.ds(offset, own), slice(None))
            send_ref[here] = send_ref[here] + mate_ref[target // 2]

            @pl.when(target != me)
            def _():
                rs_copy(index, offset, target // 2, chip).start()

    @pl.loop(0, steps)
    def _(step):
        if paired:
            project(mixed(chip, rounds - 1 - step // 2, rounds) * 2 + lax.rem(core + 1 + step, 2))
        else:
            project(mixed(me // ratio, rounds - 1 - step, rounds))

        @pl.when(step == 0)
        def _():
            all_here()

        if paired:

            @pl.when(lax.rem(step, 2) == 0)
            def _():
                forward(step // 2)

            @pl.when((lax.rem(step, 2) == 0) & (step > 0))
            def _():
                settle(step // 2 - 1)

        else:
            forward(step)

            @pl.when(step > 0)
            def _():
                settle(step - 1)

    if not paired:
        settle(rounds - 1)

    loads[6].wait()

    @pl.loop(0, points // tile)
    def _(step):
        point = step * tile + lax.broadcasted_iota(jnp.int32, (1, tile), 1)
        x_row = jnp.zeros((1, tile), F32)
        y_row = jnp.zeros((1, tile), F32)
        z_row = point.astype(F32)
        for t in range(slots):
            column = columns_ref[t]
            x = band * (NX // bands) + lax.div(column, NY)
            y = lax.rem(column, NY)
            inside = point >= t * NZ
            x_row = jnp.where(inside, x.astype(F32), x_row)
            y_row = jnp.where(inside, y.astype(F32), y_row)
            z_row = jnp.where(inside, (point - t * NZ).astype(F32), z_row)
        count = site_t_ref[:, 0:1] * x_row + site_t_ref[:, 1:2] * y_row + site_t_ref[:, 2:3] * z_row
        cosine, sine = turn_cos_sin(count, PERIOD)
        phase_ref[step, 0] = cosine
        phase_ref[step, 1] = sine

    if paired:
        settle(rounds - 1)
    total = send_ref[me // ratio, :, pl.ds(pl.multiple_of(lax.rem(me, ratio) * own, own), own), :]
    for step in range(1, chips):
        source = lax.rem(chip + step, chips)
        rs_copy(0, 0, source, source).wait_recv()
        total = total + recv_ref[source]

    total_ref[...] = jnp.zeros_like(total_ref)
    total_ref[0 : HALF * own, :] = total.reshape(HALF * own, cols)
    turned = jnp.swapaxes(total_ref[...], 0, 1)
    becp = jnp.concatenate([turned[0 : 2 * nb, : HALF * own], turned[2 * nb :, : HALF * own]], axis=1)
    scaled = becp * site_t_ref[0 : 2 * nb, 4:5]
    for d in range(NH):
        size = (NH - d) * own
        product = scaled[:, :size] * becp[:, d * own :]
        part_ref[d : d + 1, 0:size] = jnp.sum(product, axis=0, keepdims=True)

    pair_ref[...] = jnp.zeros_like(pair_ref)
    begin = 0
    for i in range(NH):
        pair_ref[begin : begin + NH - i, :] = part_ref[: NH - i, i * own : (i + 1) * own]
        begin += NH - i
    chunk = pack_ref.shape[0]
    chunks = pack_ref.shape[1] // own
    pack_ref[...] = jnp.concatenate(
        [pair_ref[q * chunk : (q + 1) * chunk, :] for q in range(chunks)], axis=1
    )

    def band_copy(step, slot):
        return pltpu.make_async_remote_copy(
            src_ref=pack_ref,
            dst_ref=band_ref.at[slot],
            send_sem=band_send.at[step],
            recv_sem=band_recv.at[slot],
            device_id=(mixed(band, step, bands), me),
            device_id_type=MESH,
        )

    for step in range(bands - 1, 0, -1):
        band_copy(step, band).start()
    summed = pack_ref[...]
    for step in range(1, bands):
        source = lax.rem(band + step, bands)
        band_copy(step, source).wait_recv()
        summed = summed + band_ref[source]
    sum_ref[...] = summed

    def ga_copy(step, slot):
        return pltpu.make_async_remote_copy(
            src_ref=sum_ref,
            dst_ref=all_ref.at[slot],
            send_sem=ga_send.at[step],
            recv_sem=ga_recv.at[slot],
            device_id=(band, mixed(me, step, groups)),
            device_id_type=MESH,
        )

    for step in range(groups - 1, 0, -1):
        ga_copy(step, me).start()
    all_ref[me] = sum_ref[...]
    for step in range(1, groups):
        ga_copy(step, lax.rem(me + step, groups)).wait_recv()
    becsum = jnp.concatenate(
        [
            jnp.concatenate([all_ref[g, :, q * own : (q + 1) * own] for g in range(groups)], axis=1)
            for q in range(chunks)
        ],
        axis=0,
    )[:pairs]
    loads[7].wait()
    even = becsum * signs_ref[:, 0:1]
    odd = becsum * signs_ref[:, 1:2]
    kind_row = small_ref[3:4, :]
    weights_ref[...] = jnp.zeros_like(weights_ref)
    for s in range(SPECIES):
        here = kind_row == float(s)
        weights_ref[s * pairs : (s + 1) * pairs, 0:atoms] = jnp.where(here, even, 0.0)
        weights_ref[s * pairs : (s + 1) * pairs, atoms : 2 * atoms] = jnp.where(here, odd, 0.0)
    weights = jnp.swapaxes(weights_ref[...], 0, 1).astype(BF16)[:, : SPECIES * pairs]

    loads[8].wait()
    for step in range(points // tile):
        coef = jnp.dot(
            weights, table_ref[:, step * tile : (step + 1) * tile], preferred_element_type=F32
        )
        real, imag = coef[:atoms], coef[atoms:]
        cosine, sine = phase_ref[step, 0], phase_ref[step, 1]
        aug_ref[0:1, step * tile : (step + 1) * tile] = jnp.sum(real * cosine + imag * sine, axis=0, keepdims=True)
        aug_ref[1:2, step * tile : (step + 1) * tile] = jnp.sum(imag * cosine - real * sine, axis=0, keepdims=True)

    lines_ref[...] = jnp.zeros_like(lines_ref)
    half = lines_ref.shape[1] // 2
    aug = aug_ref[0:2, :]
    for t in range(slots):
        lines_ref[t : t + 1, 0:NZ] = aug[0:1, t * NZ : (t + 1) * NZ]
        lines_ref[t : t + 1, half : half + NZ] = aug[1:2, t * NZ : (t + 1) * NZ]
    high, low = split(lines_ref[...])
    loads[9].wait()
    lane = lax.broadcasted_iota(jnp.int32, (slots, groups * span), 1)
    slot = lax.broadcasted_iota(jnp.int32, (slots, groups * span), 0)
    marks = jnp.zeros((slots, groups * span), F32)
    for t in range(slots):
        marks = jnp.where(slot == t, columns_ref[t].astype(F32), marks)
    both = jnp.concatenate([high, low], axis=0)
    packed = jnp.dot(both, spread_ref[0], preferred_element_type=F32)
    packed = packed[:slots] + packed[slots:] + jnp.dot(high, spread_ref[1], preferred_element_type=F32)
    packed = jnp.where(lax.rem(lane, span) == 2 * planes, marks, packed)
    for g in range(groups):
        stick_ref[g] = jnp.concatenate(
            [packed[q * rows : (q + 1) * rows, g * span : (g + 1) * span] for q in range(slots // rows)], axis=1
        )

    def stick_copy(step, target, slot):
        return pltpu.make_async_remote_copy(
            src_ref=stick_ref.at[target[1]],
            dst_ref=out_ref.at[slot],
            send_sem=dev_send.at[step],
            recv_sem=dev_recv.at[slot],
            device_id=target,
            device_id_type=MESH,
        )

    @pl.loop(0, bands - 1)
    def _(turn):
        other = mixed(band, bands - 1 - turn, bands)
        for step in range(groups):
            stick_copy(turn * groups + step, (other, lax.rem(me + step, groups)), place).start()

    for step in range(1, groups):
        stick_copy((bands - 1) * groups + step, (band, lax.rem(me + step, groups)), place).start()

    out_ref[place] = stick_ref[me]

    @pl.loop(1, devices)
    def _(step):
        stick_copy(step, (band, me), lax.rem(place + step, devices)).wait_recv()

    for slot in range(chips):
        mate_copy(0, 0, slot).wait_send()
    for step in range(1, chips):
        rs_copy(0, 0, lax.rem(chip + step, chips), chip).wait_send()
    for step in range(1, groups):
        ga_copy(step, me).wait_send()
    for step in range(1, bands):
        band_copy(step, band).wait_send()

    @pl.loop(0, devices)
    def _(step):
        @pl.when(step != (bands - 1) * groups)
        def _():
            stick_copy(step, (band, me), place).wait_send()


def finish_kernel(bands, planes, span, received_ref, out_ref, table_ref, turned_ref, angle_ref, amp_ref):
    per_row = received_ref.shape[1] // span
    total = received_ref.shape[0] * per_row
    batch = out_ref.shape[0]
    y_block = out_ref.shape[1]
    y_pad = angle_ref.shape[1]
    band = lax.axis_index("band")
    group = pl.program_id(0)

    @pl.when(group == 0)
    def _():
        received = jnp.concatenate([received_ref[:, q * span : (q + 1) * span] for q in range(per_row)], axis=0)
        turned = jnp.swapaxes(received, 0, 1)
        turned_ref[...] = turned
        column_row = turned[2 * planes : 2 * planes + 1, :]
        live_row = column_row >= 0.0
        x_row = jnp.floor((column_row + 0.5) * (1.0 / NY))
        y_row = column_row - x_row * NY
        y_values = lax.broadcasted_iota(jnp.int32, (y_pad, total), 0) + band * y_block
        cos_y, sin_y = turn_cos_sin(y_values.astype(F32) * y_row, NY)
        angle_ref[0] = jnp.where(live_row, cos_y, 0.0)
        angle_ref[1] = jnp.where(live_row, sin_y, 0.0)
        column = received[:, 2 * planes : 2 * planes + 1]
        owner = lax.rem(lax.broadcasted_iota(jnp.int32, (total, 1), 0), total // per_row) // (total // per_row // bands)
        x = jnp.floor((column + 0.5) * (1.0 / NY)) + owner.astype(F32) * (NX // bands)
        x_values = lax.broadcasted_iota(jnp.int32, (total, 256), 1).astype(F32)
        cos_x, sin_x = turn_cos_sin(x * x_values, NX)
        for part, value in enumerate(split(cos_x)):
            table_ref[part, 0:total, 0:256] = value
            table_ref[part, total : 2 * total, 256:512] = value
        for part, value in enumerate(split(sin_x)):
            table_ref[part, 0:total, 256:512] = value
            table_ref[part, total : 2 * total, 0:256] = -value

    for k in range(batch):
        real = turned_ref[pl.ds(group * batch + k, 1), :]
        imag = turned_ref[pl.ds(planes + group * batch + k, 1), :]
        cosine, sine = angle_ref[0], angle_ref[1]
        row = k * y_pad
        amp_ref[row : row + y_pad, 0:total] = (real * cosine - imag * sine).astype(BF16)
        amp_ref[row : row + y_pad, total : 2 * total] = (real * sine + imag * cosine).astype(BF16)
    amp = amp_ref[...]
    for part in range(2):
        lane = slice(256 * part, 256 * part + 256)
        result = jnp.dot(amp, table_ref[0, :, lane], preferred_element_type=F32)
        result = result + jnp.dot(amp, table_ref[1, :, lane], preferred_element_type=F32)
        for k in range(batch):
            out_ref[k, :, part, :] = result[k * y_pad : k * y_pad + y_block, 0:NX]


def on_device(
    waves, occupations, beta_table, wave_miller, atom_kinds, atom_sites, aug_table, stick_columns
):
    bands = lax.axis_size("band")
    groups = lax.axis_size("ga")
    devices = bands * groups
    atoms = atom_sites.shape[1]
    slots = stick_columns.shape[0]
    nb = waves.shape[1]
    width = waves.shape[2]
    points = aug_table.shape[1]
    planes = NZ // groups
    pairs = len(PAIR_FIRST)
    own = atoms // groups
    block = own * max(1, 32 // own)
    steps = atoms // block
    cols = 4 * nb
    tile = math.gcd(points, 256)
    lanes = 128
    span = next(n for n in (16, 32, 64, 128) if n >= 2 * planes + 1 and n * slots >= lanes)
    stick_rows = slots * span // lanes
    chunks = 128 // own
    chunk = up(-(-pairs // chunks), 8)

    odd = (ELL[PAIR_FIRST] + ELL[PAIR_SECOND]) % 2 == 1
    factors = np.where(PAIR_FIRST == PAIR_SECOND, 1.0, 2.0)
    factors = np.where((ELL[PAIR_FIRST] == 0) != (ELL[PAIR_SECOND] == 0), -factors, factors)
    signs = np.stack([np.where(odd, 0.0, factors), np.where(odd, -factors, 0.0)], axis=1).astype(np.float32)
    angle = (np.outer(np.arange(NZ), np.arange(NZ)) % NZ) * (2.0 * np.pi / NZ)
    cos_z = np.cos(angle).reshape(NZ, groups, planes)
    sin_z = np.sin(angle).reshape(NZ, groups, planes)
    half = up(NZ, 128)
    spread = np.zeros((2 * half, groups, span), np.float32)
    spread[:NZ, :, :planes] = cos_z
    spread[half : half + NZ, :, :planes] = -sin_z
    spread[:NZ, :, planes : 2 * planes] = sin_z
    spread[half : half + NZ, :, planes : 2 * planes] = cos_z
    spread = spread.reshape(2 * half, groups * span)
    spread_high = spread.astype(BF16)
    spread_low = (spread - spread_high.astype(np.float32)).astype(BF16)
    vmem = pl.BlockSpec(memory_space=pltpu.VMEM)
    hbm = pl.BlockSpec(memory_space=pl.ANY)
    dma = pltpu.SemaphoreType.DMA
    part_lanes = up(NH * own, 128)
    inputs = (
        waves,
        occupations[None, :],
        beta_table,
        wave_miller,
        atom_kinds[None, :],
        atom_sites,
        stick_columns,
        jnp.asarray(signs),
        aug_table,
        jnp.asarray(np.stack([spread_high, spread_low])),
    )
    chips = groups // 2
    received = pl.pallas_call(
        functools.partial(mega_kernel, bands, groups),
        in_specs=[hbm] * len(inputs),
        out_specs=vmem,
        out_shape=jax.ShapeDtypeStruct((devices, stick_rows, lanes), F32),
        scratch_shapes=[
            pltpu.VMEM(waves.shape, BF16),
            pltpu.VMEM((1, nb), F32),
            pltpu.VMEM(beta_table.shape, F32),
            pltpu.VMEM(wave_miller.shape, jnp.int32),
            pltpu.VMEM((1, atoms), jnp.int32),
            pltpu.VMEM(atom_sites.shape, jnp.int32),
            pltpu.SMEM((slots,), jnp.int32),
            pltpu.VMEM(signs.shape, F32),
            pltpu.VMEM((8, atoms), F32),
            pltpu.VMEM((atoms, 8), F32),
            pltpu.VMEM((HALF, 2 * SPECIES, width), F32),
            pltpu.VMEM((cols, 4 * width), BF16),
            pltpu.VMEM((HALF * block, 4 * width), BF16),
            pltpu.VMEM((steps, HALF, block, cols), F32),
            pltpu.VMEM((chips, HALF, own, cols), F32),
            pltpu.VMEM((chips, HALF, own, cols), F32),
            pltpu.VMEM((points // tile, 2, atoms, tile), F32),
            pltpu.VMEM((up(HALF * own, 128), cols), F32),
            pltpu.VMEM((up(NH, 8), part_lanes), F32),
            pltpu.VMEM((bands, chunk, chunks * own), F32),
            pltpu.VMEM((chunk * chunks, own), F32),
            pltpu.VMEM((chunk, chunks * own), F32),
            pltpu.VMEM((chunk, chunks * own), F32),
            pltpu.VMEM((groups, chunk, chunks * own), F32),
            pltpu.VMEM((up(SPECIES * pairs, 128), 2 * atoms), F32),
            pltpu.VMEM(aug_table.shape, BF16),
            pltpu.VMEM((2,) + spread.shape, BF16),
            pltpu.VMEM((8, points), F32),
            pltpu.VMEM((slots, 2 * half), F32),
            pltpu.VMEM((groups, stick_rows, lanes), F32),
            dma((chips,)),
            dma((chips,)),
            dma((chips,)),
            dma((chips,)),
            dma((bands,)),
            dma((bands,)),
            dma((groups,)),
            dma((groups,)),
            dma((devices,)),
            dma((devices,)),
            dma((len(inputs),)),
        ],
        compiler_params=pltpu.CompilerParams(collective_id=0, has_side_effects=True),
        name="slots",
    )(*inputs)
    y_block = NY // bands
    total = devices * slots
    batch = math.gcd(planes, 7)
    y_pad = up(y_block, 16)
    result = pl.pallas_call(
        functools.partial(finish_kernel, bands, planes, span),
        grid=(planes // batch,),
        in_specs=[pl.BlockSpec((devices * stick_rows, lanes), lambda g: (0, 0))],
        out_specs=pl.BlockSpec((batch, y_block, 2, NX), lambda g: (g, 0, 0, 0)),
        out_shape=jax.ShapeDtypeStruct((planes, y_block, 2, NX), F32),
        scratch_shapes=[
            pltpu.VMEM((2, 2 * total, 512), BF16),
            pltpu.VMEM((span, total), F32),
            pltpu.VMEM((2, y_pad, total), F32),
            pltpu.VMEM((batch * y_pad, 2 * total), BF16),
        ],
        name="finish",
    )(received.reshape(devices * stick_rows, lanes))
    return result.transpose(2, 0, 1, 3)


def solution(mesh):
    in_specs = (
        P(None, "band", "ga"),
        P("band"),
        P(None, "ga"),
        P(None, "ga"),
        P(),
        P(),
        P(None, ("band", "ga")),
        P(("band", "ga")),
    )
    out_specs = P(None, "ga", "band", None)
    return jax.shard_map(
        on_device, mesh=mesh, in_specs=in_specs, out_specs=out_specs, check_vma=False
    )
```

```python
import functools
import math

import jax
import jax.numpy as jnp
import numpy as np
from jax import lax
from jax.experimental import pallas as pl
from jax.experimental.pallas import tpu as pltpu
from jax.sharding import PartitionSpec as P

NX = 240
NY = 240
NZ = 224
NH = 18
HALF = NH // 2
SPECIES = 4

PERIOD = math.lcm(NX, NY, NZ)
STEP_X = PERIOD // NX
STEP_Y = PERIOD // NY
STEP_Z = PERIOD // NZ
ELL = np.array([0, 0] + [1] * 6 + [2] * 10)
PAIR_FIRST, PAIR_SECOND = np.triu_indices(NH)

highest = lax.Precision.HIGHEST
F32 = jnp.float32
BF16 = jnp.bfloat16


def fit_even(func, terms):
    nodes = 0.125 * (1.0 + np.cos(np.pi * (np.arange(64) + 0.5) / 64))
    scaled = np.polynomial.chebyshev.Chebyshev.fit(nodes, func(np.sqrt(nodes)), terms - 1, domain=[0, 0.25])
    return [float(c) for c in scaled.convert(kind=np.polynomial.Polynomial).coef]


COS_FIT = fit_even(lambda u: np.cos(2 * np.pi * u), 7)
SIN_FIT = fit_even(lambda u: np.sin(2 * np.pi * u) / u, 6)


def horner(coefs, w):
    total = jnp.full_like(w, coefs[-1])
    for c in coefs[-2::-1]:
        total = total * w + c
    return total


def turn_cos_sin(count, period):
    rest = count - jnp.round(count * (1.0 / period)) * period
    u = rest * (1.0 / period)
    w = u * u
    return horner(COS_FIT, w), u * horner(SIN_FIT, w)


MESH = pl.DeviceIdType.MESH


def greet(peers, axis_sets):
    barrier = pltpu.get_barrier_semaphore()
    for count, device_of in axis_sets:

        @pl.loop(1, count)
        def _(step):
            pl.semaphore_signal(barrier, inc=1, device_id=device_of(step), device_id_type=MESH)

    return lambda: pl.semaphore_wait(barrier, peers)


def up(value, unit):
    return -(-value // unit) * unit


def split(value):
    high = value.astype(BF16)
    return high, (value - high.astype(F32)).astype(BF16)


def mixed(value, other, count):
    if count & (count - 1):
        return lax.rem(value + other, count)
    total, bit = 0, 1
    while bit < count:
        total = total + lax.rem(value // bit + other // bit, 2) * bit
        bit *= 2
    return total


def mega_kernel(
    bands,
    groups,
    waves_hbm,
    occ_hbm,
    beta_hbm,
    miller_hbm,
    kinds_hbm,
    site_hbm,
    columns_hbm,
    signs_hbm,
    table_hbm,
    spread_hbm,
    out_ref,
    waves_ref,
    occ_ref,
    beta_ref,
    miller_ref,
    kinds_ref,
    site_ref,
    columns_ref,
    signs_ref,
    small_ref,
    site_t_ref,
    radial_ref,
    wave_ref,
    wide_ref,
    kind_ref,
    turn_ref,
    rows_ref,
    send_ref,
    mate_ref,
    recv_ref,
    phase_ref,
    total_ref,
    part_ref,
    band_ref,
    pair_ref,
    pack_ref,
    sum_ref,
    all_ref,
    weights_ref,
    table_ref,
    spread_ref,
    aug_ref,
    lines_ref,
    stick_ref,
    mate_recv,
    sent,
    came,
    local_sem,
):
    band, me = lax.axis_index("band"), lax.axis_index("ga")
    devices = bands * groups
    place = band * groups + me
    chips = groups // 2
    chip, core = me // 2, lax.rem(me, 2)
    atoms = site_ref.shape[1]
    own = atoms // groups
    width = miller_ref.shape[1]
    nb = waves_ref.shape[1]
    slots = columns_ref.shape[0]
    steps, _, block, cols = send_ref.shape
    ratio = block // own
    paired = ratio == 1
    rounds = steps // 2 if paired else steps
    units = max(1, ratio // 2)
    points = slots * NZ
    tile = phase_ref.shape[-1]
    planes = NZ // groups
    rows, lanes = stick_ref.shape[1:]
    span = lanes * rows // slots
    pairs = len(PAIR_FIRST)

    sources = (site_hbm, kinds_hbm, occ_hbm, waves_hbm, miller_hbm, beta_hbm, columns_hbm, signs_hbm, table_hbm, spread_hbm)
    targets = (site_ref, kinds_ref, occ_ref, waves_ref, miller_ref, beta_ref, columns_ref, signs_ref, table_ref, spread_ref)
    loads = [pltpu.make_async_copy(a, b, local_sem.at[n]) for n, (a, b) in enumerate(zip(sources, targets))]
    for load in loads:
        load.start()

    all_here = greet(
        groups - 1 + bands - 1,
        [
            (groups, lambda step: (band, lax.rem(me + step, groups))),
            (bands, lambda step: (lax.rem(band + step, bands), me)),
        ],
    )

    wave_ref[...] = jnp.zeros_like(wave_ref)
    small_ref[...] = jnp.zeros_like(small_ref)
    for load in loads[:3]:
        load.wait()
    small_ref[0:1, :] = site_ref[0:1, :].astype(F32) * STEP_X
    small_ref[1:2, :] = site_ref[1:2, :].astype(F32) * STEP_Y
    small_ref[2:3, :] = site_ref[2:3, :].astype(F32) * STEP_Z
    small_ref[3:4, :] = kinds_ref[...].astype(F32)
    small_ref[4:5, 0:nb] = occ_ref[...]
    small_ref[4:5, nb : 2 * nb] = occ_ref[...]
    site_t_ref[...] = jnp.swapaxes(small_ref[...], 0, 1)
    for n in range(3):
        wide_ref[n] = jnp.broadcast_to(site_t_ref[:, n : n + 1], (atoms, 128))
    kinds = jnp.broadcast_to(site_t_ref[:, 3:4], (atoms, 128)).astype(jnp.int32)
    kind_ref[0], kind_ref[1] = kinds, kinds + SPECIES

    loads[3].wait()
    re, im = waves_ref[0], waves_ref[1]
    for h in range(2):
        r, c = 2 * nb * h, 2 * width * h
        wave_ref[r : r + nb, c : c + width] = re
        wave_ref[r : r + nb, c + width : c + 2 * width] = im
        wave_ref[r + nb : r + 2 * nb, c : c + width] = im
        wave_ref[r + nb : r + 2 * nb, c + width : c + 2 * width] = -re
    loads[4].wait()
    loads[5].wait()
    for i in range(NH):
        for s in range(SPECIES):
            row = (i // HALF) * SPECIES + s
            radial_ref[i % HALF, row : row + 1, :] = beta_ref[s * NH + i : s * NH + i + 1, :]

    def located(turn, unit, own_core):
        kind = core if own_core else 1 - core
        if paired:
            target = mixed(chip, rounds - 1 - turn, rounds) * 2 + kind
            return target, 0, target
        index = mixed(me // ratio, rounds - 1 - turn, rounds)
        part = 2 * unit + kind
        return index, pl.multiple_of(part * own, own), index * ratio + part

    def all_of(kind, ref, count):
        return pltpu.make_async_remote_copy(
            src_ref=ref.at[pl.ds(0, count)],
            dst_ref=ref.at[pl.ds(0, count)],
            send_sem=sent.at[kind],
            recv_sem=came.at[kind],
            device_id=(band, me),
            device_id_type=MESH,
        )

    def mate_copy(index, offset, slot):
        return pltpu.make_async_remote_copy(
            src_ref=send_ref.at[index, :, pl.ds(offset, own), :],
            dst_ref=mate_ref.at[slot],
            send_sem=sent.at[0],
            recv_sem=mate_recv.at[slot],
            device_id=(band, chip * 2 + 1 - core),
            device_id_type=MESH,
        )

    def rs_copy(index, offset, target):
        return pltpu.make_async_remote_copy(
            src_ref=send_ref.at[index, :, pl.ds(offset, own), :],
            dst_ref=recv_ref.at[chip],
            send_sem=sent.at[1],
            recv_sem=came.at[1],
            device_id=(band, target * 2 + core),
            device_id_type=MESH,
        )

    def block_at(step):
        if paired:
            return mixed(chip, rounds - 1 - step // 2, rounds) * 2 + lax.rem(core + 1 + step, 2)
        return mixed(me // ratio, rounds - 1 - step, rounds)

    def turns(index):
        sites = [wide_ref[n, pl.ds(pl.multiple_of(index * block, block), block), :] for n in range(3)]
        sites = [jnp.concatenate([site] * (width // 128), axis=1) for site in sites]
        miller = miller_ref[...].astype(F32)
        count = sites[0] * miller[0:1, :] + sites[1] * miller[1:2, :] + sites[2] * miller[2:3, :]
        cosine, sine = turn_cos_sin(count, PERIOD)
        turn_ref[0], turn_ref[1], turn_ref[2] = cosine, -sine, sine

    def project(index, after):
        start = pl.multiple_of(index * block, block)
        kinds = [
            [kind_ref[h, pl.ds(start + q, 8), :] for q in range(0, block, 8)] for h in range(2)
        ]
        kinds = [[jnp.concatenate([kind] * (width // 128), axis=1) for kind in half] for half in kinds]
        for i in range(NH):
            radial = jnp.concatenate(
                [
                    jnp.take_along_axis(radial_ref[i % HALF], kind, axis=0, mode="promise_in_bounds")
                    for kind in kinds[i // HALF]
                ],
                axis=0,
            )
            first, second = (2, 0) if ELL[i] == 1 else (0, 1)
            row = (i % HALF) * block
            col = (i // HALF) * 2 * width
            rows_ref[row : row + block, col : col + width] = (radial * turn_ref[first]).astype(BF16)
            rows_ref[row : row + block, col + width : col + 2 * width] = (radial * turn_ref[second]).astype(BF16)
        result = lax.dot_general(
            rows_ref[...], wave_ref[...], (((1,), (1,)), ((), ())), preferred_element_type=F32
        )
        turns(after)
        send_ref[index] = result.reshape(HALF, block, cols)

    def forward(turn):
        for unit in range(units):
            index, offset, target = located(turn, unit, False)
            mate_copy(index, offset, target // 2).start()

    def settle(turn):
        for unit in range(units):
            index, offset, target = located(turn, unit, True)
            mate_copy(index, offset, target // 2).wait_recv()
            here = (index, slice(None), pl.ds(offset, own), slice(None))
            send_ref[here] = send_ref[here] + mate_ref[target // 2]

            @pl.when(target != me)
            def _():
                rs_copy(index, offset, target // 2).start()

    turns(block_at(0))

    @pl.loop(0, steps)
    def _(step):
        project(block_at(step), block_at(lax.rem(step + 1, steps)))

        @pl.when(step == 0)
        def _():
            all_here()

        if paired:

            @pl.when(lax.rem(step, 2) == 0)
            def _():
                forward(step // 2)

            @pl.when((lax.rem(step, 2) == 1) & (step < steps - 1))
            def _():
                settle(step // 2)

        else:
            forward(step)

            @pl.when(step > 0)
            def _():
                settle(step - 1)

    if not paired:
        settle(rounds - 1)

    loads[6].wait()

    @pl.loop(0, points // tile)
    def _(step):
        point = step * tile + lax.broadcasted_iota(jnp.int32, (1, tile), 1)
        x_row = jnp.zeros((1, tile), F32)
        y_row = jnp.zeros((1, tile), F32)
        z_row = point.astype(F32)
        for t in range(slots):
            column = columns_ref[t]
            x = band * (NX // bands) + lax.div(column, NY)
            y = lax.rem(column, NY)
            inside = point >= t * NZ
            x_row = jnp.where(inside, x.astype(F32), x_row)
            y_row = jnp.where(inside, y.astype(F32), y_row)
            z_row = jnp.where(inside, (point - t * NZ).astype(F32), z_row)
        count = site_t_ref[:, 0:1] * x_row + site_t_ref[:, 1:2] * y_row + site_t_ref[:, 2:3] * z_row
        cosine, sine = turn_cos_sin(count, PERIOD)
        phase_ref[step, 0] = cosine
        phase_ref[step, 1] = sine

    if paired:
        settle(rounds - 1)
    total = send_ref[me // ratio, :, pl.ds(pl.multiple_of(lax.rem(me, ratio) * own, own), own), :]
    all_of(1, recv_ref, chips - 1).wait_recv()
    for step in range(1, chips):
        total = total + recv_ref[lax.rem(chip + step, chips)]

    total_ref[...] = jnp.zeros_like(total_ref)
    total_ref[0 : HALF * own, :] = total.reshape(HALF * own, cols)
    turned = jnp.swapaxes(total_ref[...], 0, 1)
    becp = jnp.concatenate([turned[0 : 2 * nb, : HALF * own], turned[2 * nb :, : HALF * own]], axis=1)
    scaled = becp * site_t_ref[0 : 2 * nb, 4:5]
    for d in range(NH):
        size = (NH - d) * own
        product = scaled[:, :size] * becp[:, d * own :]
        part_ref[d : d + 1, 0:size] = jnp.sum(product, axis=0, keepdims=True)

    pair_ref[...] = jnp.zeros_like(pair_ref)
    begin = 0
    for i in range(NH):
        pair_ref[begin : begin + NH - i, :] = part_ref[: NH - i, i * own : (i + 1) * own]
        begin += NH - i
    chunk = pack_ref.shape[0]
    chunks = pack_ref.shape[1] // own
    pack_ref[...] = jnp.concatenate(
        [pair_ref[q * chunk : (q + 1) * chunk, :] for q in range(chunks)], axis=1
    )

    def band_copy(step):
        return pltpu.make_async_remote_copy(
            src_ref=pack_ref,
            dst_ref=band_ref.at[band],
            send_sem=sent.at[2],
            recv_sem=came.at[2],
            device_id=(mixed(band, step, bands), me),
            device_id_type=MESH,
        )

    for step in range(bands - 1, 0, -1):
        band_copy(step).start()
    summed = pack_ref[...]
    all_of(2, band_ref, bands - 1).wait_recv()
    for step in range(1, bands):
        summed = summed + band_ref[lax.rem(band + step, bands)]
    sum_ref[...] = summed

    def ga_copy(step):
        return pltpu.make_async_remote_copy(
            src_ref=sum_ref,
            dst_ref=all_ref.at[me],
            send_sem=sent.at[3],
            recv_sem=came.at[3],
            device_id=(band, mixed(me, step, groups)),
            device_id_type=MESH,
        )

    for step in range(groups - 1, 0, -1):
        ga_copy(step).start()
    all_ref[me] = sum_ref[...]
    all_of(3, all_ref, groups - 1).wait_recv()
    becsum = jnp.concatenate(
        [
            jnp.concatenate([all_ref[g, :, q * own : (q + 1) * own] for g in range(groups)], axis=1)
            for q in range(chunks)
        ],
        axis=0,
    )[:pairs]
    loads[7].wait()
    even = becsum * signs_ref[:, 0:1]
    odd = becsum * signs_ref[:, 1:2]
    kind_row = small_ref[3:4, :]
    weights_ref[...] = jnp.zeros_like(weights_ref)
    for s in range(SPECIES):
        here = kind_row == float(s)
        weights_ref[s * pairs : (s + 1) * pairs, 0:atoms] = jnp.where(here, even, 0.0)
        weights_ref[s * pairs : (s + 1) * pairs, atoms : 2 * atoms] = jnp.where(here, odd, 0.0)
    weights = jnp.swapaxes(weights_ref[...], 0, 1).astype(BF16)[:, : SPECIES * pairs]

    loads[8].wait()
    for step in range(points // tile):
        coef = jnp.dot(
            weights, table_ref[:, step * tile : (step + 1) * tile], preferred_element_type=F32
        )
        real, imag = coef[:atoms], coef[atoms:]
        cosine, sine = phase_ref[step, 0], phase_ref[step, 1]
        aug_ref[0:1, step * tile : (step + 1) * tile] = jnp.sum(real * cosine + imag * sine, axis=0, keepdims=True)
        aug_ref[1:2, step * tile : (step + 1) * tile] = jnp.sum(imag * cosine - real * sine, axis=0, keepdims=True)

    lines_ref[...] = jnp.zeros_like(lines_ref)
    half = lines_ref.shape[1] // 2
    aug = aug_ref[0:2, :]
    for t in range(slots):
        lines_ref[t : t + 1, 0:NZ] = aug[0:1, t * NZ : (t + 1) * NZ]
        lines_ref[t : t + 1, half : half + NZ] = aug[1:2, t * NZ : (t + 1) * NZ]
    high, low = split(lines_ref[...])
    loads[9].wait()
    lane = lax.broadcasted_iota(jnp.int32, (slots, groups * span), 1)
    slot = lax.broadcasted_iota(jnp.int32, (slots, groups * span), 0)
    marks = jnp.zeros((slots, groups * span), F32)
    for t in range(slots):
        marks = jnp.where(slot == t, columns_ref[t].astype(F32), marks)
    both = jnp.concatenate([high, low], axis=0)
    packed = jnp.dot(both, spread_ref[0], preferred_element_type=F32)
    packed = packed[:slots] + packed[slots:] + jnp.dot(high, spread_ref[1], preferred_element_type=F32)
    packed = jnp.where(lax.rem(lane, span) == 2 * planes, marks, packed)
    for g in range(groups):
        stick_ref[g] = jnp.concatenate(
            [packed[q * rows : (q + 1) * rows, g * span : (g + 1) * span] for q in range(slots // rows)], axis=1
        )

    def stick_copy(target):
        return pltpu.make_async_remote_copy(
            src_ref=stick_ref.at[target[1]],
            dst_ref=out_ref.at[place],
            send_sem=sent.at[4],
            recv_sem=came.at[4],
            device_id=target,
            device_id_type=MESH,
        )

    @pl.loop(0, bands - 1)
    def _(turn):
        other = mixed(band, bands - 1 - turn, bands)
        for step in range(groups):
            stick_copy((other, lax.rem(me + step, groups))).start()

    for step in range(1, groups):
        stick_copy((band, lax.rem(me + step, groups))).start()

    out_ref[place] = stick_ref[me]

    all_of(4, out_ref, devices - 1).wait_recv()

    all_of(0, mate_ref, chips).wait_send()
    all_of(1, recv_ref, chips - 1).wait_send()
    all_of(2, band_ref, bands - 1).wait_send()
    all_of(3, all_ref, groups - 1).wait_send()
    all_of(4, out_ref, devices - 1).wait_send()


def finish_kernel(bands, planes, span, received_ref, out_ref, table_ref, turned_ref, angle_ref, amp_ref):
    senders, stick_rows, lanes = received_ref.shape
    per_row = lanes // span
    total = senders * stick_rows * per_row
    batch = out_ref.shape[0]
    y_block = out_ref.shape[1]
    y_pad = angle_ref.shape[1]
    band = lax.axis_index("band")
    group = pl.program_id(0)

    @pl.when(group == 0)
    def _():
        received = received_ref[...].reshape(senders * stick_rows, lanes)
        received = jnp.concatenate([received[:, q * span : (q + 1) * span] for q in range(per_row)], axis=0)
        turned = jnp.swapaxes(received, 0, 1)
        turned_ref[...] = turned
        column_row = turned[2 * planes : 2 * planes + 1, :]
        live_row = column_row >= 0.0
        x_row = jnp.floor((column_row + 0.5) * (1.0 / NY))
        y_row = column_row - x_row * NY
        y_values = lax.broadcasted_iota(jnp.int32, (y_pad, total), 0) + band * y_block
        cos_y, sin_y = turn_cos_sin(y_values.astype(F32) * y_row, NY)
        angle_ref[0] = jnp.where(live_row, cos_y, 0.0)
        angle_ref[1] = jnp.where(live_row, sin_y, 0.0)
        column = received[:, 2 * planes : 2 * planes + 1]
        owner = lax.rem(lax.broadcasted_iota(jnp.int32, (total, 1), 0), total // per_row) // (total // per_row // bands)
        x = jnp.floor((column + 0.5) * (1.0 / NY)) + owner.astype(F32) * (NX // bands)
        x_values = lax.broadcasted_iota(jnp.int32, (total, 256), 1).astype(F32)
        cos_x, sin_x = turn_cos_sin(x * x_values, NX)
        cosine, sine = cos_x.astype(BF16), sin_x.astype(BF16)
        table_ref[0:total, 0:256] = cosine
        table_ref[total : 2 * total, 256:512] = cosine
        table_ref[0:total, 256:512] = sine
        table_ref[total : 2 * total, 0:256] = -sine

    for k in range(batch):
        real = turned_ref[pl.ds(group * batch + k, 1), :]
        imag = turned_ref[pl.ds(planes + group * batch + k, 1), :]
        cosine, sine = angle_ref[0], angle_ref[1]
        row = k * y_pad
        amp_ref[row : row + y_pad, 0:total] = (real * cosine - imag * sine).astype(BF16)
        amp_ref[row : row + y_pad, total : 2 * total] = (real * sine + imag * cosine).astype(BF16)
    amp = amp_ref[...]
    for part in range(2):
        lane = slice(256 * part, 256 * part + 256)
        result = jnp.dot(amp, table_ref[:, lane], preferred_element_type=F32)
        for k in range(batch):
            out_ref[k, :, part, :] = result[k * y_pad : k * y_pad + y_block, 0:NX]


def on_device(
    waves, occupations, beta_table, wave_miller, atom_kinds, atom_sites, aug_table, stick_columns
):
    bands = lax.axis_size("band")
    groups = lax.axis_size("ga")
    devices = bands * groups
    atoms = atom_sites.shape[1]
    slots = stick_columns.shape[0]
    nb = waves.shape[1]
    width = waves.shape[2]
    points = aug_table.shape[1]
    planes = NZ // groups
    pairs = len(PAIR_FIRST)
    own = atoms // groups
    block = own * max(1, 32 // own)
    steps = atoms // block
    cols = 4 * nb
    tile = math.gcd(points, 256)
    lanes = 128
    span = next(n for n in (16, 32, 64, 128) if n >= 2 * planes + 1 and n * slots >= lanes)
    stick_rows = slots * span // lanes
    chunks = 128 // own
    chunk = up(-(-pairs // chunks), 8)

    odd = (ELL[PAIR_FIRST] + ELL[PAIR_SECOND]) % 2 == 1
    factors = np.where(PAIR_FIRST == PAIR_SECOND, 1.0, 2.0)
    factors = np.where((ELL[PAIR_FIRST] == 0) != (ELL[PAIR_SECOND] == 0), -factors, factors)
    signs = np.stack([np.where(odd, 0.0, factors), np.where(odd, -factors, 0.0)], axis=1).astype(np.float32)
    angle = (np.outer(np.arange(NZ), np.arange(NZ)) % NZ) * (2.0 * np.pi / NZ)
    cos_z = np.cos(angle).reshape(NZ, groups, planes)
    sin_z = np.sin(angle).reshape(NZ, groups, planes)
    half = up(NZ, 128)
    spread = np.zeros((2 * half, groups, span), np.float32)
    spread[:NZ, :, :planes] = cos_z
    spread[half : half + NZ, :, :planes] = -sin_z
    spread[:NZ, :, planes : 2 * planes] = sin_z
    spread[half : half + NZ, :, planes : 2 * planes] = cos_z
    spread = spread.reshape(2 * half, groups * span)
    spread_high = spread.astype(BF16)
    spread_low = (spread - spread_high.astype(np.float32)).astype(BF16)
    vmem = pl.BlockSpec(memory_space=pltpu.VMEM)
    hbm = pl.BlockSpec(memory_space=pl.ANY)
    dma = pltpu.SemaphoreType.DMA
    part_lanes = up(NH * own, 128)
    inputs = (
        waves,
        occupations[None, :],
        beta_table,
        wave_miller,
        atom_kinds[None, :],
        atom_sites,
        stick_columns,
        jnp.asarray(signs),
        aug_table,
        jnp.asarray(np.stack([spread_high, spread_low])),
    )
    chips = groups // 2
    received = pl.pallas_call(
        functools.partial(mega_kernel, bands, groups),
        in_specs=[hbm] * len(inputs),
        out_specs=vmem,
        out_shape=pltpu.VMEM((devices, stick_rows, lanes), F32),
        scratch_shapes=[
            pltpu.VMEM(waves.shape, BF16),
            pltpu.VMEM((1, nb), F32),
            pltpu.VMEM(beta_table.shape, F32),
            pltpu.VMEM(wave_miller.shape, jnp.int32),
            pltpu.VMEM((1, atoms), jnp.int32),
            pltpu.VMEM(atom_sites.shape, jnp.int32),
            pltpu.SMEM((slots,), jnp.int32),
            pltpu.VMEM(signs.shape, F32),
            pltpu.VMEM((8, atoms), F32),
            pltpu.VMEM((atoms, 8), F32),
            pltpu.VMEM((HALF, 2 * SPECIES, width), F32),
            pltpu.VMEM((cols, 4 * width), BF16),
            pltpu.VMEM((3, atoms, 128), F32),
            pltpu.VMEM((2, atoms, 128), jnp.int32),
            pltpu.VMEM((3, block, width), F32),
            pltpu.VMEM((HALF * block, 4 * width), BF16),
            pltpu.VMEM((steps, HALF, block, cols), F32),
            pltpu.VMEM((chips, HALF, own, cols), F32),
            pltpu.VMEM((chips, HALF, own, cols), F32),
            pltpu.VMEM((points // tile, 2, atoms, tile), F32),
            pltpu.VMEM((up(HALF * own, 128), cols), F32),
            pltpu.VMEM((up(NH, 8), part_lanes), F32),
            pltpu.VMEM((bands, chunk, chunks * own), F32),
            pltpu.VMEM((chunk * chunks, own), F32),
            pltpu.VMEM((chunk, chunks * own), F32),
            pltpu.VMEM((chunk, chunks * own), F32),
            pltpu.VMEM((groups, chunk, chunks * own), F32),
            pltpu.VMEM((up(SPECIES * pairs, 128), 2 * atoms), F32),
            pltpu.VMEM(aug_table.shape, BF16),
            pltpu.VMEM((2,) + spread.shape, BF16),
            pltpu.VMEM((8, points), F32),
            pltpu.VMEM((slots, 2 * half), F32),
            pltpu.VMEM((groups, stick_rows, lanes), F32),
            dma((chips,)),
            dma((5,)),
            dma((5,)),
            dma((len(inputs),)),
        ],
        compiler_params=pltpu.CompilerParams(collective_id=0, has_side_effects=True),
        name="slots",
    )(*inputs)
    y_block = NY // bands
    total = devices * slots
    batch = math.gcd(planes, 7)
    y_pad = up(y_block, 16)
    result = pl.pallas_call(
        functools.partial(finish_kernel, bands, planes, span),
        grid=(planes // batch,),
        in_specs=[vmem],
        out_specs=pl.BlockSpec((batch, y_block, 2, NX), lambda g: (g, 0, 0, 0)),
        out_shape=jax.ShapeDtypeStruct((planes, y_block, 2, NX), F32),
        scratch_shapes=[
            pltpu.VMEM((2 * total, 512), BF16),
            pltpu.VMEM((span, total), F32),
            pltpu.VMEM((2, y_pad, total), F32),
            pltpu.VMEM((batch * y_pad, 2 * total), BF16),
        ],
        name="finish",
    )(pltpu.with_memory_space_constraint(received, pltpu.VMEM))
    return result.transpose(2, 0, 1, 3)


def solution(mesh):
    in_specs = (
        P(None, "band", "ga"),
        P("band"),
        P(None, "ga"),
        P(None, "ga"),
        P(),
        P(),
        P(None, ("band", "ga")),
        P(("band", "ga")),
    )
    out_specs = P(None, "ga", "band", None)
    return jax.shard_map(
        on_device, mesh=mesh, in_specs=in_specs, out_specs=out_specs, check_vma=False
    )
```

```python
import functools
import math

import jax
import jax.numpy as jnp
import numpy as np
from jax import lax
from jax.experimental import pallas as pl
from jax.experimental.pallas import tpu as pltpu
from jax.sharding import PartitionSpec as P

NX = 240
NY = 240
NZ = 224
NH = 18
HALF = NH // 2
SPECIES = 4

PERIOD = math.lcm(NX, NY, NZ)
STEP_X = PERIOD // NX
STEP_Y = PERIOD // NY
STEP_Z = PERIOD // NZ
ELL = np.array([0, 0] + [1] * 6 + [2] * 10)
PAIR_FIRST, PAIR_SECOND = np.triu_indices(NH)

highest = lax.Precision.HIGHEST
F32 = jnp.float32
BF16 = jnp.bfloat16


def fit_even(func, terms):
    nodes = 0.125 * (1.0 + np.cos(np.pi * (np.arange(64) + 0.5) / 64))
    scaled = np.polynomial.chebyshev.Chebyshev.fit(nodes, func(np.sqrt(nodes)), terms - 1, domain=[0, 0.25])
    return [float(c) for c in scaled.convert(kind=np.polynomial.Polynomial).coef]


COS_FIT = fit_even(lambda u: np.cos(2 * np.pi * u), 7)
SIN_FIT = fit_even(lambda u: np.sin(2 * np.pi * u) / u, 6)


def horner(coefs, w):
    total = jnp.full_like(w, coefs[-1])
    for c in coefs[-2::-1]:
        total = total * w + c
    return total


def turn_cos_sin(count, period):
    rest = count - jnp.round(count * (1.0 / period)) * period
    u = rest * (1.0 / period)
    w = u * u
    return horner(COS_FIT, w), u * horner(SIN_FIT, w)


MESH = pl.DeviceIdType.MESH


def greet(peers, axis_sets):
    barrier = pltpu.get_barrier_semaphore()
    for count, device_of in axis_sets:

        @pl.loop(1, count)
        def _(step):
            pl.semaphore_signal(barrier, inc=1, device_id=device_of(step), device_id_type=MESH)

    return lambda: pl.semaphore_wait(barrier, peers)


def up(value, unit):
    return -(-value // unit) * unit


def split(value):
    high = value.astype(BF16)
    return high, (value - high.astype(F32)).astype(BF16)


def mixed(value, other, count):
    if count & (count - 1):
        return lax.rem(value + other, count)
    total, bit = 0, 1
    while bit < count:
        total = total + lax.rem(value // bit + other // bit, 2) * bit
        bit *= 2
    return total


def mega_kernel(
    bands,
    groups,
    waves_hbm,
    occ_hbm,
    beta_hbm,
    miller_hbm,
    kinds_hbm,
    site_hbm,
    columns_hbm,
    signs_hbm,
    table_hbm,
    spread_hbm,
    out_ref,
    waves_ref,
    occ_ref,
    beta_ref,
    miller_ref,
    kinds_ref,
    site_ref,
    columns_ref,
    signs_ref,
    small_ref,
    site_t_ref,
    radial_ref,
    wave_ref,
    wide_ref,
    kind_ref,
    turn_ref,
    rows_ref,
    send_ref,
    mate_ref,
    recv_ref,
    phase_ref,
    total_ref,
    part_ref,
    band_ref,
    pair_ref,
    pack_ref,
    sum_ref,
    all_ref,
    weights_ref,
    table_ref,
    spread_ref,
    aug_ref,
    lines_ref,
    stick_ref,
    mate_recv,
    sent,
    came,
    local_sem,
):
    band, me = lax.axis_index("band"), lax.axis_index("ga")
    devices = bands * groups
    place = band * groups + me
    chips = groups // 2
    chip, core = me // 2, lax.rem(me, 2)
    atoms = site_ref.shape[1]
    own = atoms // groups
    width = miller_ref.shape[1]
    nb = waves_ref.shape[1]
    slots = columns_ref.shape[0]
    steps, _, block, cols = send_ref.shape
    ratio = block // own
    paired = ratio == 1
    rounds = steps // 2 if paired else steps
    units = max(1, ratio // 2)
    points = slots * NZ
    tile = phase_ref.shape[-1]
    planes = NZ // groups
    rows, lanes = stick_ref.shape[1:]
    span = lanes * rows // slots
    pairs = len(PAIR_FIRST)

    sources = (site_hbm, kinds_hbm, occ_hbm, waves_hbm, miller_hbm, beta_hbm, columns_hbm, signs_hbm, table_hbm, spread_hbm)
    targets = (site_ref, kinds_ref, occ_ref, waves_ref, miller_ref, beta_ref, columns_ref, signs_ref, table_ref, spread_ref)
    loads = [pltpu.make_async_copy(a, b, local_sem.at[n]) for n, (a, b) in enumerate(zip(sources, targets))]
    for load in loads:
        load.start()

    all_here = greet(
        groups - 1 + bands - 1,
        [
            (groups, lambda step: (band, lax.rem(me + step, groups))),
            (bands, lambda step: (lax.rem(band + step, bands), me)),
        ],
    )

    wave_ref[...] = jnp.zeros_like(wave_ref)
    small_ref[...] = jnp.zeros_like(small_ref)
    for load in loads[:3]:
        load.wait()
    small_ref[0:1, :] = site_ref[0:1, :].astype(F32) * STEP_X
    small_ref[1:2, :] = site_ref[1:2, :].astype(F32) * STEP_Y
    small_ref[2:3, :] = site_ref[2:3, :].astype(F32) * STEP_Z
    small_ref[3:4, :] = kinds_ref[...].astype(F32)
    small_ref[4:5, 0:nb] = occ_ref[...]
    small_ref[4:5, nb : 2 * nb] = occ_ref[...]
    site_t_ref[...] = jnp.swapaxes(small_ref[...], 0, 1)
    for n in range(3):
        wide_ref[n] = jnp.broadcast_to(site_t_ref[:, n : n + 1], (atoms, 128))
    kinds = jnp.broadcast_to(site_t_ref[:, 3:4], (atoms, 128)).astype(jnp.int32)
    kind_ref[0], kind_ref[1] = kinds, kinds + SPECIES

    loads[3].wait()
    re, im = waves_ref[0], waves_ref[1]
    for h in range(2):
        r, c = 2 * nb * h, 2 * width * h
        wave_ref[r : r + nb, c : c + width] = re
        wave_ref[r : r + nb, c + width : c + 2 * width] = im
        wave_ref[r + nb : r + 2 * nb, c : c + width] = im
        wave_ref[r + nb : r + 2 * nb, c + width : c + 2 * width] = -re
    loads[4].wait()
    loads[5].wait()
    for i in range(NH):
        for s in range(SPECIES):
            row = (i // HALF) * SPECIES + s
            radial_ref[i % HALF, row : row + 1, :] = beta_ref[s * NH + i : s * NH + i + 1, :]

    def located(turn, unit, own_core):
        kind = core if own_core else 1 - core
        if paired:
            target = mixed(chip, rounds - 1 - turn, rounds) * 2 + kind
            return target, 0, target
        index = mixed(me // ratio, rounds - 1 - turn, rounds)
        part = 2 * unit + kind
        return index, pl.multiple_of(part * own, own), index * ratio + part

    def all_of(kind, ref, count):
        return pltpu.make_async_remote_copy(
            src_ref=ref.at[pl.ds(0, count)],
            dst_ref=ref.at[pl.ds(0, count)],
            send_sem=sent.at[kind],
            recv_sem=came.at[kind],
            device_id=(band, me),
            device_id_type=MESH,
        )

    def mate_copy(index, offset, slot):
        return pltpu.make_async_remote_copy(
            src_ref=send_ref.at[index, :, pl.ds(offset, own), :],
            dst_ref=mate_ref.at[slot],
            send_sem=sent.at[0],
            recv_sem=mate_recv.at[slot],
            device_id=(band, chip * 2 + 1 - core),
            device_id_type=MESH,
        )

    def rs_copy(index, offset, target):
        return pltpu.make_async_remote_copy(
            src_ref=send_ref.at[index, :, pl.ds(offset, own), :],
            dst_ref=recv_ref.at[chip],
            send_sem=sent.at[1],
            recv_sem=came.at[1],
            device_id=(band, target * 2 + core),
            device_id_type=MESH,
        )

    def block_at(step):
        if paired:
            return mixed(chip, rounds - 1 - step // 2, rounds) * 2 + lax.rem(core + 1 + step, 2)
        return mixed(me // ratio, rounds - 1 - step, rounds)

    def turns(index):
        sites = [wide_ref[n, pl.ds(pl.multiple_of(index * block, block), block), :] for n in range(3)]
        sites = [jnp.concatenate([site] * (width // 128), axis=1) for site in sites]
        miller = miller_ref[...].astype(F32)
        count = sites[0] * miller[0:1, :] + sites[1] * miller[1:2, :] + sites[2] * miller[2:3, :]
        cosine, sine = turn_cos_sin(count, PERIOD)
        turn_ref[0], turn_ref[1], turn_ref[2] = cosine, -sine, sine

    def project(index, after):
        start = pl.multiple_of(index * block, block)
        kinds = [
            [kind_ref[h, pl.ds(start + q, 8), :] for q in range(0, block, 8)] for h in range(2)
        ]
        kinds = [[jnp.concatenate([kind] * (width // 128), axis=1) for kind in half] for half in kinds]
        for i in range(NH):
            radial = jnp.concatenate(
                [
                    jnp.take_along_axis(radial_ref[i % HALF], kind, axis=0, mode="promise_in_bounds")
                    for kind in kinds[i // HALF]
                ],
                axis=0,
            )
            first, second = (2, 0) if ELL[i] == 1 else (0, 1)
            row = (i % HALF) * block
            col = (i // HALF) * 2 * width
            rows_ref[row : row + block, col : col + width] = (radial * turn_ref[first]).astype(BF16)
            rows_ref[row : row + block, col + width : col + 2 * width] = (radial * turn_ref[second]).astype(BF16)
        result = lax.dot_general(
            rows_ref[...], wave_ref[...], (((1,), (1,)), ((), ())), preferred_element_type=F32
        )
        turns(after)
        send_ref[index] = result.reshape(HALF, block, cols)

    def forward(turn):
        for unit in range(units):
            index, offset, target = located(turn, unit, False)
            mate_copy(index, offset, target // 2).start()

    def settle(turn):
        for unit in range(units):
            index, offset, target = located(turn, unit, True)
            mate_copy(index, offset, target // 2).wait_recv()
            here = (index, slice(None), pl.ds(offset, own), slice(None))
            send_ref[here] = send_ref[here] + mate_ref[target // 2]

            @pl.when(target != me)
            def _():
                rs_copy(index, offset, target // 2).start()

    turns(block_at(0))

    @pl.loop(0, steps)
    def _(step):
        project(block_at(step), block_at(lax.rem(step + 1, steps)))

        @pl.when(step == 0)
        def _():
            all_here()

        if paired:

            @pl.when(lax.rem(step, 2) == 0)
            def _():
                forward(step // 2)

            @pl.when((lax.rem(step, 2) == 1) & (step < steps - 1))
            def _():
                settle(step // 2)

        else:
            forward(step)

            @pl.when(step > 0)
            def _():
                settle(step - 1)

    if not paired:
        settle(rounds - 1)

    loads[6].wait()

    @pl.loop(0, points // tile)
    def _(step):
        point = step * tile + lax.broadcasted_iota(jnp.int32, (1, tile), 1)
        x_row = jnp.zeros((1, tile), F32)
        y_row = jnp.zeros((1, tile), F32)
        z_row = point.astype(F32)
        for t in range(slots):
            column = columns_ref[t]
            x = band * (NX // bands) + lax.div(column, NY)
            y = lax.rem(column, NY)
            inside = point >= t * NZ
            x_row = jnp.where(inside, x.astype(F32), x_row)
            y_row = jnp.where(inside, y.astype(F32), y_row)
            z_row = jnp.where(inside, (point - t * NZ).astype(F32), z_row)
        count = site_t_ref[:, 0:1] * x_row + site_t_ref[:, 1:2] * y_row + site_t_ref[:, 2:3] * z_row
        cosine, sine = turn_cos_sin(count, PERIOD)
        phase_ref[step, 0] = cosine
        phase_ref[step, 1] = sine

    if paired:
        settle(rounds - 1)
    total = send_ref[me // ratio, :, pl.ds(pl.multiple_of(lax.rem(me, ratio) * own, own), own), :]
    all_of(1, recv_ref, chips - 1).wait_recv()
    for step in range(1, chips):
        total = total + recv_ref[lax.rem(chip + step, chips)]

    total_ref[...] = jnp.zeros_like(total_ref)
    total_ref[0 : HALF * own, :] = total.reshape(HALF * own, cols)
    turned = jnp.swapaxes(total_ref[...], 0, 1)
    becp = jnp.concatenate([turned[0 : 2 * nb, : HALF * own], turned[2 * nb :, : HALF * own]], axis=1)
    scaled = becp * site_t_ref[0 : 2 * nb, 4:5]
    for d in range(NH):
        size = (NH - d) * own
        product = scaled[:, :size] * becp[:, d * own :]
        part_ref[d : d + 1, 0:size] = jnp.sum(product, axis=0, keepdims=True)

    pair_ref[...] = jnp.zeros_like(pair_ref)
    begin = 0
    for i in range(NH):
        pair_ref[begin : begin + NH - i, :] = part_ref[: NH - i, i * own : (i + 1) * own]
        begin += NH - i
    chunk = pack_ref.shape[0]
    chunks = pack_ref.shape[1] // own
    pack_ref[...] = jnp.concatenate(
        [pair_ref[q * chunk : (q + 1) * chunk, :] for q in range(chunks)], axis=1
    )

    halves = 2 if chunk % 16 == 0 else 1
    share = chunk // halves

    def band_copy(step, part):
        return pltpu.make_async_remote_copy(
            src_ref=pack_ref.at[pl.ds(part * share, share)],
            dst_ref=band_ref.at[part, band],
            send_sem=sent.at[2 + part],
            recv_sem=came.at[2 + part],
            device_id=(mixed(band, step, bands), me),
            device_id_type=MESH,
        )

    def ga_copy(step, part):
        return pltpu.make_async_remote_copy(
            src_ref=sum_ref.at[pl.ds(part * share, share)],
            dst_ref=all_ref.at[part, me],
            send_sem=sent.at[4 + part],
            recv_sem=came.at[4 + part],
            device_id=(band, mixed(me, step, groups)),
            device_id_type=MESH,
        )

    for part in range(halves):
        for step in range(bands - 1, 0, -1):
            band_copy(step, part).start()
    for part in range(halves):
        rows_here = slice(part * share, (part + 1) * share)
        summed = pack_ref[rows_here, :]
        all_of(2 + part, band_ref.at[part], bands - 1).wait_recv()
        for step in range(1, bands):
            summed = summed + band_ref[part, lax.rem(band + step, bands)]
        sum_ref[rows_here, :] = summed
        all_ref[part, me] = summed
        for step in range(groups - 1, 0, -1):
            ga_copy(step, part).start()
    for part in range(halves):
        all_of(4 + part, all_ref.at[part], groups - 1).wait_recv()
    becsum = jnp.concatenate(
        [
            jnp.concatenate([all_ref[part, g, :, q * own : (q + 1) * own] for g in range(groups)], axis=1)
            for q in range(chunks)
            for part in range(halves)
        ],
        axis=0,
    )[:pairs]
    loads[7].wait()
    even = becsum * signs_ref[:, 0:1]
    odd = becsum * signs_ref[:, 1:2]
    kind_row = small_ref[3:4, :]
    weights_ref[...] = jnp.zeros_like(weights_ref)
    for s in range(SPECIES):
        here = kind_row == float(s)
        weights_ref[s * pairs : (s + 1) * pairs, 0:atoms] = jnp.where(here, even, 0.0)
        weights_ref[s * pairs : (s + 1) * pairs, atoms : 2 * atoms] = jnp.where(here, odd, 0.0)
    weights = jnp.swapaxes(weights_ref[...], 0, 1).astype(BF16)[:, : SPECIES * pairs]

    loads[8].wait()
    for step in range(points // tile):
        coef = jnp.dot(
            weights, table_ref[:, step * tile : (step + 1) * tile], preferred_element_type=F32
        )
        real, imag = coef[:atoms], coef[atoms:]
        cosine, sine = phase_ref[step, 0], phase_ref[step, 1]
        aug_ref[0:1, step * tile : (step + 1) * tile] = jnp.sum(real * cosine + imag * sine, axis=0, keepdims=True)
        aug_ref[1:2, step * tile : (step + 1) * tile] = jnp.sum(imag * cosine - real * sine, axis=0, keepdims=True)

    lines_ref[...] = jnp.zeros_like(lines_ref)
    half = lines_ref.shape[1] // 2
    aug = aug_ref[0:2, :]
    for t in range(slots):
        lines_ref[t : t + 1, 0:NZ] = aug[0:1, t * NZ : (t + 1) * NZ]
        lines_ref[t : t + 1, half : half + NZ] = aug[1:2, t * NZ : (t + 1) * NZ]
    high, low = split(lines_ref[...])
    loads[9].wait()
    lane = lax.broadcasted_iota(jnp.int32, (slots, groups * span), 1)
    slot = lax.broadcasted_iota(jnp.int32, (slots, groups * span), 0)
    marks = jnp.zeros((slots, groups * span), F32)
    for t in range(slots):
        marks = jnp.where(slot == t, columns_ref[t].astype(F32), marks)
    both = jnp.concatenate([high, low], axis=0)
    packed = jnp.dot(both, spread_ref[0], preferred_element_type=F32)
    packed = packed[:slots] + packed[slots:] + jnp.dot(high, spread_ref[1], preferred_element_type=F32)
    packed = jnp.where(lax.rem(lane, span) == 2 * planes, marks, packed)
    for g in range(groups):
        stick_ref[g] = jnp.concatenate(
            [packed[q * rows : (q + 1) * rows, g * span : (g + 1) * span] for q in range(slots // rows)], axis=1
        )

    def stick_copy(target):
        return pltpu.make_async_remote_copy(
            src_ref=stick_ref.at[target[1]],
            dst_ref=out_ref.at[place],
            send_sem=sent.at[6],
            recv_sem=came.at[6],
            device_id=target,
            device_id_type=MESH,
        )

    @pl.loop(0, bands - 1)
    def _(turn):
        other = mixed(band, bands - 1 - turn, bands)
        for step in range(groups):
            stick_copy((other, lax.rem(me + step, groups))).start()

    for step in range(1, groups):
        stick_copy((band, lax.rem(me + step, groups))).start()

    out_ref[place] = stick_ref[me]

    all_of(6, out_ref, devices - 1).wait_recv()

    all_of(0, mate_ref, chips).wait_send()
    all_of(1, recv_ref, chips - 1).wait_send()
    for part in range(halves):
        all_of(2 + part, band_ref.at[part], bands - 1).wait_send()
        all_of(4 + part, all_ref.at[part], groups - 1).wait_send()
    all_of(6, out_ref, devices - 1).wait_send()


def finish_kernel(bands, planes, span, received_ref, out_hbm, table_ref, turned_ref, angle_ref, amp_ref, out_ref, sem):
    senders, stick_rows, lanes = received_ref.shape
    per_row = lanes // span
    total = senders * stick_rows * per_row
    _, batch, y_block, _, _ = out_ref.shape
    y_pad = angle_ref.shape[1]
    band = lax.axis_index("band")

    received = received_ref[...].reshape(senders * stick_rows, lanes)
    received = jnp.concatenate([received[:, q * span : (q + 1) * span] for q in range(per_row)], axis=0)
    turned = jnp.swapaxes(received, 0, 1)
    turned_ref[...] = turned
    column_row = turned[2 * planes : 2 * planes + 1, :]
    live_row = column_row >= 0.0
    x_row = jnp.floor((column_row + 0.5) * (1.0 / NY))
    y_row = column_row - x_row * NY
    y_values = lax.broadcasted_iota(jnp.int32, (y_pad, total), 0) + band * y_block
    cos_y, sin_y = turn_cos_sin(y_values.astype(F32) * y_row, NY)
    angle_ref[0] = jnp.where(live_row, cos_y, 0.0)
    angle_ref[1] = jnp.where(live_row, sin_y, 0.0)
    column = received[:, 2 * planes : 2 * planes + 1]
    owner = lax.rem(lax.broadcasted_iota(jnp.int32, (total, 1), 0), total // per_row) // (total // per_row // bands)
    x = jnp.floor((column + 0.5) * (1.0 / NY)) + owner.astype(F32) * (NX // bands)
    x_values = lax.broadcasted_iota(jnp.int32, (total, 256), 1).astype(F32)
    cos_x, sin_x = turn_cos_sin(x * x_values, NX)
    cosine, sine = cos_x.astype(BF16), sin_x.astype(BF16)
    table_ref[0:total, 0:256] = cosine
    table_ref[total : 2 * total, 256:512] = cosine
    table_ref[0:total, 256:512] = sine
    table_ref[total : 2 * total, 0:256] = -sine

    def copy(n):
        return pltpu.make_async_copy(out_ref.at[n % 2], out_hbm.at[pl.ds(n * batch, batch)], sem.at[n % 2])

    for n in range(planes // batch):
        for k in range(batch):
            plane = n * batch + k
            real, imag = turned_ref[plane : plane + 1, :], turned_ref[planes + plane : planes + plane + 1, :]
            cosine, sine = angle_ref[0], angle_ref[1]
            row = k * y_pad
            amp_ref[row : row + y_pad, 0:total] = (real * cosine - imag * sine).astype(BF16)
            amp_ref[row : row + y_pad, total : 2 * total] = (real * sine + imag * cosine).astype(BF16)
        amp = amp_ref[...]
        if n >= 2:
            copy(n - 2).wait()
        for part in range(2):
            result = jnp.dot(amp, table_ref[:, 256 * part : 256 * part + 256], preferred_element_type=F32)
            for k in range(batch):
                out_ref[n % 2, k, :, part, :] = result[k * y_pad : k * y_pad + y_block, 0:NX]
        copy(n).start()
    for n in range(max(0, planes // batch - 2), planes // batch):
        copy(n).wait()


def on_device(
    waves, occupations, beta_table, wave_miller, atom_kinds, atom_sites, aug_table, stick_columns
):
    bands = lax.axis_size("band")
    groups = lax.axis_size("ga")
    devices = bands * groups
    atoms = atom_sites.shape[1]
    slots = stick_columns.shape[0]
    nb = waves.shape[1]
    width = waves.shape[2]
    points = aug_table.shape[1]
    planes = NZ // groups
    pairs = len(PAIR_FIRST)
    own = atoms // groups
    block = own * max(1, 32 // own)
    steps = atoms // block
    cols = 4 * nb
    tile = math.gcd(points, 256)
    lanes = 128
    span = next(n for n in (16, 32, 64, 128) if n >= 2 * planes + 1 and n * slots >= lanes)
    stick_rows = slots * span // lanes
    chunks = 128 // own
    chunk = up(-(-pairs // chunks), 8)
    halves = 2 if chunk % 16 == 0 else 1

    odd = (ELL[PAIR_FIRST] + ELL[PAIR_SECOND]) % 2 == 1
    factors = np.where(PAIR_FIRST == PAIR_SECOND, 1.0, 2.0)
    factors = np.where((ELL[PAIR_FIRST] == 0) != (ELL[PAIR_SECOND] == 0), -factors, factors)
    signs = np.stack([np.where(odd, 0.0, factors), np.where(odd, -factors, 0.0)], axis=1).astype(np.float32)
    angle = (np.outer(np.arange(NZ), np.arange(NZ)) % NZ) * (2.0 * np.pi / NZ)
    cos_z = np.cos(angle).reshape(NZ, groups, planes)
    sin_z = np.sin(angle).reshape(NZ, groups, planes)
    half = up(NZ, 128)
    spread = np.zeros((2 * half, groups, span), np.float32)
    spread[:NZ, :, :planes] = cos_z
    spread[half : half + NZ, :, :planes] = -sin_z
    spread[:NZ, :, planes : 2 * planes] = sin_z
    spread[half : half + NZ, :, planes : 2 * planes] = cos_z
    spread = spread.reshape(2 * half, groups * span)
    spread_high = spread.astype(BF16)
    spread_low = (spread - spread_high.astype(np.float32)).astype(BF16)
    vmem = pl.BlockSpec(memory_space=pltpu.VMEM)
    hbm = pl.BlockSpec(memory_space=pl.ANY)
    dma = pltpu.SemaphoreType.DMA
    part_lanes = up(NH * own, 128)
    inputs = (
        waves,
        occupations[None, :],
        beta_table,
        wave_miller,
        atom_kinds[None, :],
        atom_sites,
        stick_columns,
        jnp.asarray(signs),
        aug_table,
        jnp.asarray(np.stack([spread_high, spread_low])),
    )
    chips = groups // 2
    received = pl.pallas_call(
        functools.partial(mega_kernel, bands, groups),
        in_specs=[hbm] * len(inputs),
        out_specs=vmem,
        out_shape=pltpu.VMEM((devices, stick_rows, lanes), F32),
        scratch_shapes=[
            pltpu.VMEM(waves.shape, BF16),
            pltpu.VMEM((1, nb), F32),
            pltpu.VMEM(beta_table.shape, F32),
            pltpu.VMEM(wave_miller.shape, jnp.int32),
            pltpu.VMEM((1, atoms), jnp.int32),
            pltpu.VMEM(atom_sites.shape, jnp.int32),
            pltpu.SMEM((slots,), jnp.int32),
            pltpu.VMEM(signs.shape, F32),
            pltpu.VMEM((8, atoms), F32),
            pltpu.VMEM((atoms, 8), F32),
            pltpu.VMEM((HALF, 2 * SPECIES, width), F32),
            pltpu.VMEM((cols, 4 * width), BF16),
            pltpu.VMEM((3, atoms, 128), F32),
            pltpu.VMEM((2, atoms, 128), jnp.int32),
            pltpu.VMEM((3, block, width), F32),
            pltpu.VMEM((HALF * block, 4 * width), BF16),
            pltpu.VMEM((steps, HALF, block, cols), F32),
            pltpu.VMEM((chips, HALF, own, cols), F32),
            pltpu.VMEM((chips, HALF, own, cols), F32),
            pltpu.VMEM((points // tile, 2, atoms, tile), F32),
            pltpu.VMEM((up(HALF * own, 128), cols), F32),
            pltpu.VMEM((up(NH, 8), part_lanes), F32),
            pltpu.VMEM((halves, bands, chunk // halves, chunks * own), F32),
            pltpu.VMEM((chunk * chunks, own), F32),
            pltpu.VMEM((chunk, chunks * own), F32),
            pltpu.VMEM((chunk, chunks * own), F32),
            pltpu.VMEM((halves, groups, chunk // halves, chunks * own), F32),
            pltpu.VMEM((up(SPECIES * pairs, 128), 2 * atoms), F32),
            pltpu.VMEM(aug_table.shape, BF16),
            pltpu.VMEM((2,) + spread.shape, BF16),
            pltpu.VMEM((8, points), F32),
            pltpu.VMEM((slots, 2 * half), F32),
            pltpu.VMEM((groups, stick_rows, lanes), F32),
            dma((chips,)),
            dma((7,)),
            dma((7,)),
            dma((len(inputs),)),
        ],
        compiler_params=pltpu.CompilerParams(collective_id=0, has_side_effects=True),
        name="slots",
    )(*inputs)
    y_block = NY // bands
    total = devices * slots
    batch = math.gcd(planes, 14)
    y_pad = up(y_block, 16)
    result = pl.pallas_call(
        functools.partial(finish_kernel, bands, planes, span),
        in_specs=[vmem],
        out_specs=hbm,
        out_shape=jax.ShapeDtypeStruct((planes, y_block, 2, NX), F32),
        scratch_shapes=[
            pltpu.VMEM((2 * total, 512), BF16),
            pltpu.VMEM((span, total), F32),
            pltpu.VMEM((2, y_pad, total), F32),
            pltpu.VMEM((batch * y_pad, 2 * total), BF16),
            pltpu.VMEM((2, batch, y_block, 2, NX), F32),
            dma((2,)),
        ],
        name="finish",
    )(pltpu.with_memory_space_constraint(received, pltpu.VMEM))
    return result.transpose(2, 0, 1, 3)


def solution(mesh):
    in_specs = (
        P(None, "band", "ga"),
        P("band"),
        P(None, "ga"),
        P(None, "ga"),
        P(),
        P(),
        P(None, ("band", "ga")),
        P(("band", "ga")),
    )
    out_specs = P(None, "ga", "band", None)
    return jax.shard_map(
        on_device, mesh=mesh, in_specs=in_specs, out_specs=out_specs, check_vma=False
    )
```
